16 devices in a mesh: rep: 4 (over y, z, core), dp: 4 (over x).
Axes of the slice: x: 4, y: 2, z: 1, core: 2. Of those that a mesh axis runs over, the one named last changes fastest.
The devices are a block of a 4x4x8 slice.
Arguments:
- x: bfloat16 [16, 1024, 1024], P(('rep', 'dp')), parts along dimension 0
- dy: bfloat16 [16, 1024, 1024], P(('rep', 'dp')), parts along dimension 0
- w_gate: bfloat16 [2, 1024, 3200], replicated
- w_up: bfloat16 [2, 1024, 3200], replicated
- w_down: bfloat16 [2, 3200, 1024], replicated
- m_w_gate: float32 [2, 1024, 3200], replicated
- m_w_up: float32 [2, 1024, 3200], replicated
- m_w_down: float32 [2, 3200, 1024], replicated
- v_w_gate: float32 [2, 1024, 3200], replicated
- v_w_up: float32 [2, 1024, 3200], replicated
- v_w_down: float32 [2, 3200, 1024], replicated
Outputs:
- output 1: bfloat16 [8, 1024, 3200], P('rep'), parts along dimension 0
- output 2: bfloat16 [8, 1024, 3200], P('rep'), parts along dimension 0
- output 3: bfloat16 [8, 3200, 1024], P('rep'), parts along dimension 0
- output 4: float32 [8, 1024, 3200], P('rep'), parts along dimension 0
- output 5: float32 [8, 1024, 3200], P('rep'), parts along dimension 0
- output 6: float32 [8, 3200, 1024], P('rep'), parts along dimension 0
- output 7: float32 [8, 1024, 3200], P('rep'), parts along dimension 0
- output 8: float32 [8, 1024, 3200], P('rep'), parts along dimension 0
- output 9: float32 [8, 3200, 1024], P('rep'), parts along dimension 0
There are 4 independent parts. The reference program is written for one: setup_inputs(seed, part) draws one part's arguments, and reference() takes and returns one part's arrays. A program takes and returns all parts, laid end to end along the dimension named above; an argument that names none is the same for every part.
All inputs are finite; a program needn't handle non-finite values.
Results may differ from the reference program's by a relative error of at most 0.022.
Values are sent between devices in bfloat16 or wider.
A program may use at most 768 MiB of HBM per device.

```python
import jax
import jax.numpy as jnp
from jax import lax

SEQUENCES = 4
TOKENS = 1024
D = 1024
FF = 3200
LAYERS = 2
NAMES = ("w_gate", "w_up", "w_down")
SHAPES = {"w_gate": (LAYERS, D, FF), "w_up": (LAYERS, D, FF), "w_down": (LAYERS, FF, D)}


def bump(key, n, height):
    away = (jnp.arange(n, dtype=jnp.int32) - jax.random.randint(key, (), 0, n, jnp.int32)) % n
    return jnp.where(away < n // 8, height, 1.0)


def together(key, own, strength):
    shared = jax.random.normal(key, own.shape[1:], jnp.float32)
    return (own + strength * shared) * lax.rsqrt(1 + strength * strength)


def setup_inputs(seed: int = 0, part: int = 0) -> dict:
    kx, kdy, ka, kb, kz, kf, kh, kl, *keys = jax.random.split(jax.random.key(seed), 8 + 3 * len(NAMES))
    kx, kdy, ka, kb = (jax.random.fold_in(k, part) for k in (kx, kdy, ka, kb))
    kw, km, kv = (keys[i::3] for i in range(3))
    shape = (SEQUENCES, TOKENS, D)
    much_x, much_dy = jax.random.uniform(kz, (2,), jnp.float32, 0.0, 1.0)
    loud = 2.0 ** jax.random.uniform(jax.random.fold_in(kz, 1), (), jnp.float32, -1.0, 2.0)
    layers = 2.0 ** jax.random.uniform(kl, (LAYERS, 1, 1), jnp.float32, -1.0, 1.0)
    x = together(ka, jax.random.normal(kx, shape, jnp.float32), much_x) * bump(kf, D, 4.0)
    dy = together(kb, jax.random.normal(kdy, shape, jnp.float32), much_dy)
    drawn = {"x": x.astype(jnp.bfloat16), "dy": (loud * dy * (SEQUENCES * TOKENS) ** -0.5).astype(jnp.bfloat16)}
    for key, name in zip(kw, NAMES, strict=True):
        w = jax.random.normal(key, SHAPES[name], jnp.float32) * SHAPES[name][1] ** -0.5
        drawn[name] = (w * {"w_gate": 1.0, "w_up": bump(kh, FF, 4.0), "w_down": layers}[name]).astype(jnp.bfloat16)
    for key, name in zip(km, NAMES, strict=True):
        drawn[f"m_{name}"] = 0.1 * jax.random.normal(key, SHAPES[name], jnp.float32)
    for key, name in zip(kv, NAMES, strict=True):
        drawn[f"v_{name}"] = jax.random.uniform(key, SHAPES[name], jnp.float32, 0.005, 0.015)
    return drawn


def matmul(a, w):
    return jnp.dot(a, w, preferred_element_type=jnp.float32).astype(jnp.bfloat16)


def normed(h):
    wide = h.astype(jnp.float32)
    scale = lax.rsqrt(jnp.mean(wide**2, -1, keepdims=True) + 1e-6)
    return (wide * scale).astype(jnp.bfloat16)


def layer(h, w):
    a = normed(h)
    gate = jnp.dot(a, w["w_gate"], preferred_element_type=jnp.float32)
    up = jnp.dot(a, w["w_up"], preferred_element_type=jnp.float32)
    return h + matmul((jax.nn.silu(gate) * up).astype(jnp.bfloat16), w["w_down"])


def adamw(w, m, v, g):
    m = 0.9 * m + 0.1 * g
    v = 0.95 * v + 0.05 * g * g
    step = m * lax.rsqrt(v + 1e-8) + 0.1 * w
    return (w - 0.02 * step).astype(jnp.bfloat16), m, v


def stack(weights, h):
    return lax.scan(lambda h, w: (layer(h, w), None), h, weights)[0]


def reference(x, dy, w_gate, w_up, w_down, m_w_gate, m_w_up, m_w_down, v_w_gate, v_w_up, v_w_down):
    weights = dict(zip(NAMES, (w_gate, w_up, w_down), strict=True))

    def take(so_far, sequence):
        h, by_y = sequence
        _, back = jax.vjp(lambda w: stack(w, h), weights)
        return jax.tree.map(lambda total, term: total + term.astype(jnp.float32), so_far, back(by_y)[0]), None

    none_yet = {name: jnp.zeros(w.shape, jnp.float32) for name, w in weights.items()}
    by_weights, _ = lax.scan(take, none_yet, (x, dy))
    gradients = [by_weights[name].astype(jnp.bfloat16).astype(jnp.float32) for name in NAMES]
    new = [
        adamw(w.astype(jnp.float32), m, v, g)
        for w, m, v, g in zip((w_gate, w_up, w_down), (m_w_gate, m_w_up, m_w_down), (v_w_gate, v_w_up, v_w_down), gradients, strict=True)
    ]
    return tuple(one[which] for which in range(3) for one in new)
```

```python
import functools

import jax
import jax.numpy as jnp
from jax import lax
from jax.experimental import pallas as pl
from jax.experimental.pallas import tpu as pltpu
from jax.sharding import PartitionSpec as P

F32, BF16 = jnp.float32, jnp.bfloat16
NT = (((1,), (1,)), ((), ()))


def adam_store(g, w, m_ref, v_ref, w_out, m_out, v_out):
    m = 0.9 * m_ref[0] + 0.1 * g
    v = 0.95 * v_ref[0] + 0.05 * g * g
    w_out[0] = (w - 0.02 * (m * lax.rsqrt(v + 1e-8) + 0.1 * w)).astype(BF16)
    m_out[0] = m
    v_out[0] = v


def kernel(parts, chunk, n_out, aliased, a, dh, wg, wu, wd, mg, mu, md, vg, vu, vd, *rest):
    rest = rest[aliased:]
    wgo, wuo, wdo, mgo, muo, mdo, vgo, vuo, vdo, wgt, wut, hid, dgt, dut = rest
    s = pl.program_id(1)
    tokens = a.shape[0] // parts

    @pl.when(s == 0)
    def _():
        wgt[...] = wg[0].T
        wut[...] = wu[0].T

    @pl.when(s < parts)
    def _():
        def one(i, _):
            rows = pl.ds(pl.multiple_of(s * tokens + i * chunk, chunk), chunk)
            ac, dc = a[rows, :], dh[rows, :]
            g = lax.dot_general(wgt[...], ac, NT, preferred_element_type=F32)
            u = lax.dot_general(wut[...], ac, NT, preferred_element_type=F32)
            d = lax.dot_general(wd[0], dc, NT, preferred_element_type=F32).astype(BF16).astype(F32)
            sig = 1.0 / (1.0 + jnp.exp(-g))
            silu = g * sig
            hid[:, rows] = (silu * u).astype(BF16)
            dut[:, rows] = (d * silu).astype(BF16)
            dgt[:, rows] = (d * u * (sig + silu * (1.0 - sig))).astype(BF16)
            return 0

        lax.fori_loop(0, tokens // chunk, one, 0)

    @pl.when(s >= parts)
    def _():
        n = pl.multiple_of((s - parts) * n_out, n_out)
        cols = pl.ds(n, n_out)
        ac, dc = a[:, cols], dh[:, cols]
        g = jnp.dot(dgt[...], ac, preferred_element_type=F32)
        adam_store(g.T.astype(BF16).astype(F32), wg[0, cols, :].astype(F32), mg, vg, wgo, mgo, vgo)
        g = jnp.dot(dut[...], ac, preferred_element_type=F32)
        adam_store(g.T.astype(BF16).astype(F32), wu[0, cols, :].astype(F32), mu, vu, wuo, muo, vuo)
        g = jnp.dot(hid[...], dc, preferred_element_type=F32)
        adam_store(g.astype(BF16).astype(F32), wd[0, :, cols].astype(F32), md, vd, wdo, mdo, vdo)


def layer_step(number, a, dh, w, m, v, done=None, ffb=640, parts=2, chunk=512, n_out=256):
    rows, d = a.shape
    ff = w[0].shape[2]
    chunks = d // n_out
    late = lambda s: jnp.maximum(s - parts, 0)
    whole = pl.BlockSpec((rows, d), lambda f, s: (0, 0), pipeline_mode=pl.Buffered(1))
    w_in = [pl.BlockSpec((1, d, ffb), lambda f, s: (number, 0, f))] * 2 + [pl.BlockSpec((1, ffb, d), lambda f, s: (number, f, 0))]
    tile = [pl.BlockSpec((1, n_out, ffb), lambda f, s: (number, late(s), f))] * 2 + [
        pl.BlockSpec((1, ffb, n_out), lambda f, s: (number, f, late(s)))
    ]
    out_shape = [jax.ShapeDtypeStruct(x.shape, x.dtype) for x in (*w, *m, *v)]
    extra = list(done) if done is not None else []
    return pl.pallas_call(
        functools.partial(kernel, parts, chunk, n_out, len(extra)),
        grid=(ff // ffb, parts + chunks),
        in_specs=[whole, whole] + w_in + tile + tile + [pl.BlockSpec(memory_space=pl.ANY)] * len(extra),
        out_specs=tile * 3,
        out_shape=out_shape,
        scratch_shapes=[pltpu.VMEM((ffb, d), BF16)] * 2 + [pltpu.VMEM((ffb, rows), BF16)] * 3,
        input_output_aliases={11 + i: i for i in range(len(extra))},
        compiler_params=pltpu.CompilerParams(vmem_limit_bytes=67_043_328, dimension_semantics=("arbitrary", "arbitrary")),
        cost_estimate=pl.CostEstimate(flops=12 * rows * d * ff, bytes_accessed=20 * 3 * d * ff, transcendentals=0),
        name=f"layer_step_{number}",
    )(a, dh, *w, *m, *v, *extra)


def matmul(a, w):
    return jnp.dot(a, w, preferred_element_type=F32).astype(BF16)


def matmul_t(a, w):
    return lax.dot_general(a, w, NT, preferred_element_type=F32).astype(BF16)


def scale_of(h):
    wide = h.astype(F32)
    return lax.rsqrt(jnp.mean(wide**2, -1, keepdims=True) + 1e-6)


def own_chain(x, dy, w):
    (gate0, gate1), (up0, up1), (down0, down1) = w
    a0 = (x.astype(F32) * scale_of(x)).astype(BF16)
    g, u = jnp.dot(a0, gate0, preferred_element_type=F32), jnp.dot(a0, up0, preferred_element_type=F32)
    h = x + matmul((jax.nn.silu(g) * u).astype(BF16), down0)
    scale = scale_of(h)
    wide = h.astype(F32)
    a1 = (wide * scale).astype(BF16)
    return a0, h, a1, scale


def own_back(h, a, scale, dy, gate, up, down):
    g, u = jnp.dot(a, gate, preferred_element_type=F32), jnp.dot(a, up, preferred_element_type=F32)
    d = matmul_t(dy, down).astype(F32)
    sig = jax.nn.sigmoid(g)
    silu = g * sig
    da = matmul_t((d * u * (sig + silu * (1.0 - sig))).astype(BF16), gate) + matmul_t((d * silu).astype(BF16), up)
    wide, da = h.astype(F32), da.astype(F32)
    back = da * scale - wide * (scale * scale * scale) * jnp.mean(da * wide, -1, keepdims=True)
    return dy + back.astype(BF16)


def solution(mesh):
    def step(x, dy, *arrays):
        w, m, v = (arrays[i : i + 3] for i in (0, 3, 6))
        x, dy = x[0], dy[0]
        gather = lambda one: lax.all_gather(one, "dp", tiled=True)
        pairs = tuple((one[0], one[1]) for one in w)
        a0, h1, a1, scale = own_chain(x, dy, pairs)
        dy_all = gather(dy)
        a1_all = gather(a1)
        a0, _ = lax.optimization_barrier((a0, a1))
        a0_all = gather(a0)
        dh1 = own_back(h1, a1, scale, dy, *(one[1] for one in w))
        dh1_all = gather(dh1)
        new = layer_step(1, a1_all, dy_all, w, m, v)
        return tuple(layer_step(0, a0_all, dh1_all, w, m, v, done=new))

    return jax.shard_map(
        step,
        mesh=mesh,
        in_specs=(P(("rep", "dp"), None, None),) * 2 + (P(None, None, None),) * 9,
        out_specs=(P("rep", None, None),) * 9,
        check_vma=False,
    )
```

```python
import functools

import jax
import jax.numpy as jnp
from jax import lax
from jax.experimental import pallas as pl
from jax.experimental.pallas import tpu as pltpu
from jax.sharding import PartitionSpec as P


F32, BF16 = jnp.float32, jnp.bfloat16
NT = (((1,), (1,)), ((), ()))
TN = (((0,), (0,)), ((), ()))


def adam_store(g, w, m_ref, v_ref, w_out, m_out, v_out):
    g = g.astype(BF16).astype(F32)
    m = 0.9 * m_ref[0] + 0.1 * g
    v = 0.95 * v_ref[0] + 0.05 * g * g
    w_out[0] = (w.astype(F32) - 0.02 * (m * lax.rsqrt(v + 1e-8) + 0.1 * w.astype(F32))).astype(BF16)
    m_out[0] = m
    v_out[0] = v


def layer_kernel(pieces, tokens, chunk, n_out, bases, extra, *refs):
    a_all, dh_all, wg, wu, wd, mg, mu, md, vg, vu, vd = refs[:11]
    base = refs[11 : 11 + bases]
    rest = refs[11 + bases + extra :]
    wgo, wuo, wdo, mgo, muo, mdo, vgo, vuo, vdo, a, dh, wgt, wut, hid, dgt, dut, sem = rest
    f, s = pl.program_id(0), pl.program_id(1)
    size = tokens
    a_at, dh_at = pieces

    def source(i):
        return pl.ds(pl.multiple_of(i * size, size), size)

    def copies(i):
        rows = pl.ds(pl.multiple_of(i * size, size), size)
        return (
            pltpu.make_async_copy(a_all.at[source(a_at(i))], a.at[rows], sem.at[0, i]),
            pltpu.make_async_copy(dh_all.at[source(dh_at(i))], dh.at[rows], sem.at[1, i]),
        )

    @pl.when((f == 0) & (s == 0))
    def _():
        for i in range(a.shape[0] // size):
            for copy in copies(i):
                copy.start()

    @pl.when(s == 0)
    def _():
        wgt[...] = wg[0].T
        wut[...] = wu[0].T

        def one(i, _):
            @pl.when((f == 0) & (lax.rem(i, size // chunk) == 0))
            def _():
                for copy in copies(lax.div(i, size // chunk)):
                    copy.wait()

            rows = pl.ds(pl.multiple_of(i * chunk, chunk), chunk)
            ac, dc = a[rows, :], dh[rows, :]
            g = lax.dot_general(wgt[...], ac, NT, preferred_element_type=F32)
            u = lax.dot_general(wut[...], ac, NT, preferred_element_type=F32)
            d = lax.dot_general(wd[0], dc, NT, preferred_element_type=F32).astype(BF16).astype(F32)
            sig = 1.0 / (1.0 + jnp.exp(-g))
            silu = g * sig
            hid[:, rows] = (silu * u).astype(BF16)
            dut[:, rows] = (d * silu).astype(BF16)
            dgt[:, rows] = (d * u * (sig + silu * (1.0 - sig))).astype(BF16)
            return 0

        lax.fori_loop(0, a.shape[0] // chunk, one, 0)

    @pl.when(s >= 1)
    def _():
        cols = pl.ds(pl.multiple_of((s - 1) * n_out, n_out), n_out)
        ac, dc = a[:, cols], dh[:, cols]
        g = jnp.dot(dgt[...], ac, preferred_element_type=F32).T
        adam_store(g + base[0][...] if bases else g, wg[0, cols, :], mg, vg, wgo, mgo, vgo)
        g = jnp.dot(dut[...], ac, preferred_element_type=F32).T
        adam_store(g + base[1][...] if bases else g, wu[0, cols, :], mu, vu, wuo, muo, vuo)
        g = jnp.dot(hid[...], dc, preferred_element_type=F32)
        adam_store(g + base[2][...] if bases else g, wd[0, :, cols], md, vd, wdo, mdo, vdo)


def layer_step(number, a, dh, pieces, w, m, v, done=None, base=None, skip=0, after=(), ffb=640, chunk=256, n_out=256):
    count, size, *maps = pieces
    d = a.shape[1]
    rows = count * size
    ff = w[0].shape[2] - skip * ffb
    chunks = d // n_out
    late = lambda s: jnp.maximum(s - 1, 0)
    apart = pl.BlockSpec(memory_space=pl.ANY)
    w_in = [pl.BlockSpec((1, d, ffb), lambda f, s: (number, 0, f + skip))] * 2 + [
        pl.BlockSpec((1, ffb, d), lambda f, s: (number, f + skip, 0))
    ]
    tile = [pl.BlockSpec((1, n_out, ffb), lambda f, s: (number, late(s), f + skip))] * 2 + [
        pl.BlockSpec((1, ffb, n_out), lambda f, s: (number, f + skip, late(s)))
    ]
    flat = [pl.BlockSpec((n_out, ffb), lambda f, s: (late(s), f))] * 2 + [pl.BlockSpec((ffb, n_out), lambda f, s: (f, late(s)))]
    out_shape = [jax.ShapeDtypeStruct(x.shape, x.dtype) for x in (*w, *m, *v)]
    base, extra, after = list(base or []), list(done or []), list(after)
    first = 11 + len(base)
    return pl.pallas_call(
        functools.partial(layer_kernel, maps, size, chunk, n_out, len(base), len(extra) + len(after)),
        grid=(ff // ffb, chunks + 1),
        in_specs=[apart] * 2 + w_in + tile + tile + flat[: len(base)] + [apart] * (len(extra) + len(after)),
        out_specs=tile * 3,
        out_shape=out_shape,
        scratch_shapes=[pltpu.VMEM((rows, d), BF16)] * 2
        + [pltpu.VMEM((ffb, d), BF16)] * 2
        + [pltpu.VMEM((ffb, rows), BF16)] * 3
        + [pltpu.SemaphoreType.DMA((2, count))],
        input_output_aliases={first + i: i for i in range(len(extra))},
        compiler_params=pltpu.CompilerParams(vmem_limit_bytes=67_043_328, dimension_semantics=("arbitrary", "arbitrary")),
        cost_estimate=pl.CostEstimate(flops=12 * rows * d * ff, bytes_accessed=20 * 3 * d * ff, transcendentals=0),
    )(a, dh, *w, *m, *v, *base, *extra, *after)


def part_kernel(chunk, n_out, a_all, dh_all, wgt, wut, wd, out, a, dh, hid, dgt, dut, sem):
    count = sem.shape[1]
    size = a.shape[0] // count

    def copies(i):
        rows = pl.ds(pl.multiple_of(i * size, size), size)
        return (
            pltpu.make_async_copy(a_all.at[rows], a.at[rows], sem.at[0, i]),
            pltpu.make_async_copy(dh_all.at[rows], dh.at[rows], sem.at[1, i]),
        )

    for i in range(count):
        for copy in copies(i):
            copy.start()

    def one(i, _):
        @pl.when(lax.rem(i, size // chunk) == 0)
        def _():
            for copy in copies(lax.div(i, size // chunk)):
                copy.wait()

        rows = pl.ds(pl.multiple_of(i * chunk, chunk), chunk)
        ac, dc = a[rows, :], dh[rows, :]
        g = lax.dot_general(wgt[...], ac, NT, preferred_element_type=F32)
        u = lax.dot_general(wut[...], ac, NT, preferred_element_type=F32)
        d = lax.dot_general(wd[...], dc, NT, preferred_element_type=F32).astype(BF16).astype(F32)
        sig = 1.0 / (1.0 + jnp.exp(-g))
        silu = g * sig
        hid[:, rows] = (silu * u).astype(BF16)
        dut[:, rows] = (d * silu).astype(BF16)
        dgt[:, rows] = (d * u * (sig + silu * (1.0 - sig))).astype(BF16)
        return 0

    lax.fori_loop(0, a.shape[0] // chunk, one, 0)
    each = wgt.shape[0]

    def two(i, _):
        cols = pl.ds(pl.multiple_of(i * n_out, n_out), n_out)
        ac, dc = a[:, cols], dh[:, cols]
        out[0:each, cols] = jnp.dot(dgt[...], ac, preferred_element_type=F32).astype(BF16)
        out[each : 2 * each, cols] = jnp.dot(dut[...], ac, preferred_element_type=F32).astype(BF16)
        out[2 * each : 3 * each, cols] = jnp.dot(hid[...], dc, preferred_element_type=F32).astype(BF16)
        return 0

    lax.fori_loop(0, a.shape[1] // n_out, two, 0)


def part_grads(a, dh, wgt, wut, wd, pieces, chunk=512, n_out=256):
    rows, d = a.shape
    each = wgt.shape[0]
    inside = pl.BlockSpec(memory_space=pltpu.VMEM)
    return pl.pallas_call(
        functools.partial(part_kernel, chunk, n_out),
        in_specs=[pl.BlockSpec(memory_space=pl.ANY)] * 2 + [inside] * 3,
        out_specs=inside,
        out_shape=jax.ShapeDtypeStruct((3 * each, d), BF16),
        scratch_shapes=[pltpu.VMEM((rows, d), BF16)] * 2 + [pltpu.VMEM((each, rows), BF16)] * 3 + [pltpu.SemaphoreType.DMA((2, pieces))],
        compiler_params=pltpu.CompilerParams(vmem_limit_bytes=67_043_328),
        cost_estimate=pl.CostEstimate(flops=12 * rows * d * each, bytes_accessed=4 * rows * d, transcendentals=0),
        name="part_grads",
    )(a, dh, wgt, wut, wd)


def update_kernel(extra, *refs):
    grads, (wg, wu, wd, mg, mu, md, vg, vu, vd), outs = refs[:6], refs[6:15], refs[15 + extra :]
    wgo, wuo, wdo, mgo, muo, mdo, vgo, vuo, vdo = outs
    g, u, d = (jnp.concatenate([grads[2 * i][...], grads[2 * i + 1][...]]).astype(F32) for i in range(3))
    adam_store(g.T, wg[0], mg, vg, wgo, mgo, vgo)
    adam_store(u.T, wu[0], mu, vu, wuo, muo, vuo)
    adam_store(d, wd[0], md, vd, wdo, mdo, vdo)


def update_step(number, grads, w, m, v, done, blocks, ffb=640, n_out=256):
    each, d = ffb // 2, grads.shape[1]
    parts = [pl.BlockSpec((each, n_out), lambda f, s, i=i, j=j: ((2 * f + j) * 3 + i, s)) for i in range(3) for j in range(2)]
    tile = [pl.BlockSpec((1, n_out, ffb), lambda f, s: (number, s, f))] * 2 + [pl.BlockSpec((1, ffb, n_out), lambda f, s: (number, f, s))]
    return pl.pallas_call(
        functools.partial(update_kernel, len(done)),
        grid=(blocks, d // n_out),
        in_specs=parts + tile * 3 + [pl.BlockSpec(memory_space=pl.ANY)] * len(done),
        out_specs=tile * 3,
        out_shape=[jax.ShapeDtypeStruct(x.shape, x.dtype) for x in (*w, *m, *v)],
        input_output_aliases={15 + i: i for i in range(len(done))},
        compiler_params=pltpu.CompilerParams(vmem_limit_bytes=67_043_328, dimension_semantics=("arbitrary", "arbitrary")),
        cost_estimate=pl.CostEstimate(flops=60 * blocks * d * ffb, bytes_accessed=66 * blocks * d * ffb, transcendentals=0),
    )(*[grads] * 6, *w, *m, *v, *done)


def matmul(a, w):
    return jnp.dot(a, w, preferred_element_type=F32).astype(BF16)


def matmul_t(a, w):
    return lax.dot_general(a, w, NT, preferred_element_type=F32).astype(BF16)


def scale_of(h):
    wide = h.astype(F32)
    return lax.rsqrt(jnp.mean(wide**2, -1, keepdims=True) + 1e-6)


def own_chain(x, w):
    (gate0, gate1), (up0, up1), (down0, down1) = w
    a0 = (x.astype(F32) * scale_of(x)).astype(BF16)
    g, u = jnp.dot(a0, gate0, preferred_element_type=F32), jnp.dot(a0, up0, preferred_element_type=F32)
    h = x + matmul((jax.nn.silu(g) * u).astype(BF16), down0)
    scale = scale_of(h)
    wide = h.astype(F32)
    a1 = (wide * scale).astype(BF16)
    return a0, h, a1, scale


def own_back(h, a, scale, dy, gate, up, down):
    g, u = jnp.dot(a, gate, preferred_element_type=F32), jnp.dot(a, up, preferred_element_type=F32)
    d = matmul_t(dy, down).astype(F32)
    sig = jax.nn.sigmoid(g)
    silu = g * sig
    dg, du, hidden = (d * u * (sig + silu * (1.0 - sig))).astype(BF16), (d * silu).astype(BF16), (silu * u).astype(BF16)
    da = matmul_t(dg, gate) + matmul_t(du, up)
    wide, da = h.astype(F32), da.astype(F32)
    back = da * scale - wide * (scale * scale * scale) * jnp.mean(da * wide, -1, keepdims=True)
    parts = [lax.dot_general(one, other, TN, preferred_element_type=F32) for one, other in ((a, dg), (a, du), (hidden, dy))]
    return dy + back.astype(BF16), parts


BLOCK, SHARED = 640, 2


def solution(mesh):
    n = mesh.shape["dp"]
    assert SHARED * BLOCK // n * 2 == BLOCK

    def step(x, dy, *arrays):
        w, m, v = (arrays[i : i + 3] for i in (0, 3, 6))
        x, dy = x[0], dy[0]

        def gather(one):
            return lax.all_gather(one, "dp", tiled=True)

        pairs = tuple((one[0], one[1]) for one in w)
        a0, h1, a1, scale = own_chain(x, pairs)
        dy_all = gather(dy)
        a1_all = gather(a1)
        dh1, parts = own_back(h1, a1, scale, dy, *(one[1] for one in w))
        a0, _ = lax.optimization_barrier((a0, a1))
        a0_all, dh1_all = gather(a0), gather(dh1)
        others = lambda i: lax.rem(lax.axis_index("dp") + 1 + i, n)
        each = SHARED * BLOCK // n
        start = lax.axis_index("dp") * each
        gate, up = (lax.dynamic_slice(one, (0, 0, start), (1, one.shape[1], each))[0].T for one in w[:2])
        down = lax.dynamic_slice(w[2], (0, start, 0), (1, each, w[2].shape[2]))[0]
        new = layer_step(1, a1_all, dy_all, (n - 1, x.shape[0], others, others), w, m, v, base=parts)
        a0_all, *new = lax.optimization_barrier((a0_all, *new))
        mine = part_grads(a0_all, dh1_all, gate, up, down, n)
        grads = gather(mine)
        whole = (n, x.shape[0], lambda i: i, lambda i: i)
        new = layer_step(0, a0_all, dh1_all, whole, w, m, v, done=new, skip=SHARED, after=(mine,))
        return tuple(update_step(0, grads, w, m, v, new, SHARED))

    return jax.shard_map(
        step,
        mesh=mesh,
        in_specs=(P(("rep", "dp"), None, None),) * 2 + (P(None, None, None),) * 9,
        out_specs=(P("rep", None, None),) * 9,
        check_vma=False,
    )
```

```python
import functools

import jax
import jax.numpy as jnp
from jax import lax
from jax.experimental import pallas as pl
from jax.experimental.pallas import tpu as pltpu
from jax.sharding import PartitionSpec as P


F32, BF16 = jnp.float32, jnp.bfloat16
NT = (((1,), (1,)), ((), ()))


def adam_store(g, w, m_ref, v_ref, w_out, m_out, v_out):
    g = g.astype(BF16).astype(F32)
    m = 0.9 * m_ref[0] + 0.1 * g
    v = 0.95 * v_ref[0] + 0.05 * g * g
    w_out[0] = (w.astype(F32) - 0.02 * (m * lax.rsqrt(v + 1e-8) + 0.1 * w.astype(F32))).astype(BF16)
    m_out[0] = m
    v_out[0] = v


def layer_kernel(pieces, tokens, chunk, n_out, bases, extra, *refs):
    a_all, dh_all, wgt, wut, wg, wu, wd, mg, mu, md, vg, vu, vd = refs[:13]
    base = refs[13 : 13 + bases]
    rest = refs[13 + bases + extra :]
    wgo, wuo, wdo, mgo, muo, mdo, vgo, vuo, vdo, a, dh, hid, dgt, dut, sem = rest
    f, s = pl.program_id(0), pl.program_id(1)
    size = tokens
    a_at, dh_at = pieces

    def source(i):
        return pl.ds(pl.multiple_of(i * size, size), size)

    def copies(i):
        rows = pl.ds(pl.multiple_of(i * size, size), size)
        return (
            pltpu.make_async_copy(a_all.at[source(a_at(i))], a.at[rows], sem.at[0, i]),
            pltpu.make_async_copy(dh_all.at[source(dh_at(i))], dh.at[rows], sem.at[1, i]),
        )

    @pl.when((f == 0) & (s == 0))
    def _():
        for i in range(a.shape[0] // size):
            for copy in copies(i):
                copy.start()

    @pl.when(s == 0)
    def _():
        def one(i, _):
            @pl.when((f == 0) & (lax.rem(i, size // chunk) == 0))
            def _():
                for copy in copies(lax.div(i, size // chunk)):
                    copy.wait()

            rows = pl.ds(pl.multiple_of(i * chunk, chunk), chunk)
            ac, dc = a[rows, :], dh[rows, :]
            g = lax.dot_general(wgt[...], ac, NT, preferred_element_type=F32)
            u = lax.dot_general(wut[...], ac, NT, preferred_element_type=F32)
            d = lax.dot_general(wd[0], dc, NT, preferred_element_type=F32).astype(BF16).astype(F32)
            sig = 1.0 / (1.0 + jnp.exp(-g))
            silu = g * sig
            hid[:, rows] = (silu * u).astype(BF16)
            dut[:, rows] = (d * silu).astype(BF16)
            dgt[:, rows] = (d * u * (sig + silu * (1.0 - sig))).astype(BF16)
            return 0

        lax.fori_loop(0, a.shape[0] // chunk, one, 0)

    @pl.when(s >= 1)
    def _():
        cols = pl.ds(pl.multiple_of((s - 1) * n_out, n_out), n_out)
        ac, dc = a[:, cols], dh[:, cols]
        g = jnp.dot(dgt[...], ac, preferred_element_type=F32).T
        adam_store(g + base[0][...] if bases else g, wg[0], mg, vg, wgo, mgo, vgo)
        g = jnp.dot(dut[...], ac, preferred_element_type=F32).T
        adam_store(g + base[1][...] if bases else g, wu[0], mu, vu, wuo, muo, vuo)
        g = jnp.dot(hid[...], dc, preferred_element_type=F32)
        adam_store(g + base[2][...] if bases else g, wd[0, :, cols], md, vd, wdo, mdo, vdo)


def layer_step(number, a, dh, pieces, turned, w, m, v, done=None, base=None, skip=0, after=(), ffb=640, chunk=1024, n_out=256):
    count, size, *maps = pieces
    d = a.shape[1]
    rows = count * size
    ff = w[0].shape[2] - skip * ffb
    chunks = d // n_out
    late = lambda s: jnp.maximum(s - 1, 0)
    apart = pl.BlockSpec(memory_space=pl.ANY)
    tile = [pl.BlockSpec((1, n_out, ffb), lambda f, s: (number, late(s), f + skip))] * 2 + [
        pl.BlockSpec((1, ffb, n_out), lambda f, s: (number, f + skip, late(s)))
    ]
    flat = [pl.BlockSpec((n_out, ffb), lambda f, s: (late(s), f + skip))] * 2 + [
        pl.BlockSpec((ffb, n_out), lambda f, s: (f + skip, late(s)))
    ]
    out_shape = [jax.ShapeDtypeStruct(x.shape, x.dtype) for x in (*w, *m, *v)]
    base, extra, after = list(base or []), list(done or []), list(after)
    first = 13 + len(base)
    return pl.pallas_call(
        functools.partial(layer_kernel, maps, size, chunk, n_out, len(base), len(extra) + len(after)),
        grid=(ff // ffb, chunks + 1),
        in_specs=[apart] * 2
        + [pl.BlockSpec((ffb, d), lambda f, s: (f + skip, 0))] * 2
        + tile[:2]
        + [pl.BlockSpec((1, ffb, d), lambda f, s: (number, f + skip, 0))]
        + tile * 2
        + flat[: len(base)] + [apart] * (len(extra) + len(after)),
        out_specs=tile * 3,
        out_shape=out_shape,
        scratch_shapes=[pltpu.VMEM((rows, d), BF16)] * 2
        + [pltpu.VMEM((ffb, rows), BF16)] * 3
        + [pltpu.SemaphoreType.DMA((2, count))],
        input_output_aliases={first + i: i for i in range(len(extra))},
        compiler_params=pltpu.CompilerParams(vmem_limit_bytes=67_043_328, dimension_semantics=("arbitrary", "arbitrary")),
        cost_estimate=pl.CostEstimate(flops=12 * rows * d * ff, bytes_accessed=20 * 3 * d * ff, transcendentals=0),
    )(a, dh, *turned, *w, *m, *v, *base, *extra, *after)


def part_kernel(chunk, n_out, a_all, dh_all, wgt, wut, wd, out, a, dh, hid, dgt, dut, sem):
    count = sem.shape[1]
    size = a.shape[0] // count

    def copies(i):
        rows = pl.ds(pl.multiple_of(i * size, size), size)
        return (
            pltpu.make_async_copy(a_all.at[rows], a.at[rows], sem.at[0, i]),
            pltpu.make_async_copy(dh_all.at[rows], dh.at[rows], sem.at[1, i]),
        )

    for i in range(count):
        for copy in copies(i):
            copy.start()

    def one(i, _):
        @pl.when(lax.rem(i, size // chunk) == 0)
        def _():
            for copy in copies(lax.div(i, size // chunk)):
                copy.wait()

        rows = pl.ds(pl.multiple_of(i * chunk, chunk), chunk)
        ac, dc = a[rows, :], dh[rows, :]
        g = lax.dot_general(wgt[...], ac, NT, preferred_element_type=F32)
        u = lax.dot_general(wut[...], ac, NT, preferred_element_type=F32)
        d = lax.dot_general(wd[...], dc, NT, preferred_element_type=F32).astype(BF16).astype(F32)
        sig = 1.0 / (1.0 + jnp.exp(-g))
        silu = g * sig
        hid[:, rows] = (silu * u).astype(BF16)
        dut[:, rows] = (d * silu).astype(BF16)
        dgt[:, rows] = (d * u * (sig + silu * (1.0 - sig))).astype(BF16)
        return 0

    lax.fori_loop(0, a.shape[0] // chunk, one, 0)
    each = wgt.shape[0]

    def two(i, _):
        cols = pl.ds(pl.multiple_of(i * n_out, n_out), n_out)
        ac, dc = a[:, cols], dh[:, cols]
        out[0:each, cols] = jnp.dot(dgt[...], ac, preferred_element_type=F32).astype(BF16)
        out[each : 2 * each, cols] = jnp.dot(dut[...], ac, preferred_element_type=F32).astype(BF16)
        out[2 * each : 3 * each, cols] = jnp.dot(hid[...], dc, preferred_element_type=F32).astype(BF16)
        return 0

    lax.fori_loop(0, a.shape[1] // n_out, two, 0)


def part_grads(a, dh, wgt, wut, wd, pieces, chunk=512, n_out=1024):
    rows, d = a.shape
    each = wgt.shape[0]
    inside = pl.BlockSpec(memory_space=pltpu.VMEM)
    return pl.pallas_call(
        functools.partial(part_kernel, chunk, n_out),
        in_specs=[pl.BlockSpec(memory_space=pl.ANY)] * 2 + [inside] * 3,
        out_specs=inside,
        out_shape=jax.ShapeDtypeStruct((3 * each, d), BF16),
        scratch_shapes=[pltpu.VMEM((rows, d), BF16)] * 2 + [pltpu.VMEM((each, rows), BF16)] * 3 + [pltpu.SemaphoreType.DMA((2, pieces))],
        compiler_params=pltpu.CompilerParams(vmem_limit_bytes=67_043_328),
        cost_estimate=pl.CostEstimate(flops=12 * rows * d * each, bytes_accessed=4 * rows * d, transcendentals=0),
        name="part_grads",
    )(a, dh, wgt, wut, wd)


def update_kernel(extra, *refs):
    grads, (wg, wu, wd, mg, mu, md, vg, vu, vd), outs = refs[:6], refs[6:15], refs[15 + extra :]
    wgo, wuo, wdo, mgo, muo, mdo, vgo, vuo, vdo = outs
    g, u, d = (jnp.concatenate([grads[2 * i][...], grads[2 * i + 1][...]]).astype(F32) for i in range(3))
    adam_store(g.T, wg[0], mg, vg, wgo, mgo, vgo)
    adam_store(u.T, wu[0], mu, vu, wuo, muo, vuo)
    adam_store(d, wd[0], md, vd, wdo, mdo, vdo)


def update_step(number, grads, w, m, v, done, blocks, ffb=640, n_out=256):
    each, d = ffb // 2, grads.shape[1]
    parts = [pl.BlockSpec((each, n_out), lambda f, s, i=i, j=j: ((2 * f + j) * 3 + i, s)) for i in range(3) for j in range(2)]
    tile = [pl.BlockSpec((1, n_out, ffb), lambda f, s: (number, s, f))] * 2 + [pl.BlockSpec((1, ffb, n_out), lambda f, s: (number, f, s))]
    return pl.pallas_call(
        functools.partial(update_kernel, len(done)),
        grid=(blocks, d // n_out),
        in_specs=parts + tile * 3 + [pl.BlockSpec(memory_space=pl.ANY)] * len(done),
        out_specs=tile * 3,
        out_shape=[jax.ShapeDtypeStruct(x.shape, x.dtype) for x in (*w, *m, *v)],
        input_output_aliases={15 + i: i for i in range(len(done))},
        compiler_params=pltpu.CompilerParams(vmem_limit_bytes=67_043_328, dimension_semantics=("arbitrary", "arbitrary")),
        cost_estimate=pl.CostEstimate(flops=60 * blocks * d * ffb, bytes_accessed=66 * blocks * d * ffb, transcendentals=0),
    )(*[grads] * 6, *w, *m, *v, *done)


def own_kernel(chunk, n_out, a, dh, wg, wu, wd, pg, pu, pd, *rest):
    wgt, wut, *da, hid, dgt, dut = rest
    wgt[...] = wg[0].T
    wut[...] = wu[0].T

    if da:

        @pl.when(pl.program_id(0) == 0)
        def _():
            da[0][...] = jnp.zeros_like(da[0])

    def one(i, _):
        rows = pl.ds(pl.multiple_of(i * chunk, chunk), chunk)
        ac, dc = a[rows, :], dh[rows, :]
        g = lax.dot_general(wgt[...], ac, NT, preferred_element_type=F32)
        u = lax.dot_general(wut[...], ac, NT, preferred_element_type=F32)
        d = lax.dot_general(wd[0], dc, NT, preferred_element_type=F32).astype(BF16).astype(F32)
        sig = 1.0 / (1.0 + jnp.exp(-g))
        silu = g * sig
        hid[:, rows] = (silu * u).astype(BF16)
        du, dg = (d * silu).astype(BF16), (d * u * (sig + silu * (1.0 - sig))).astype(BF16)
        dut[:, rows] = du
        dgt[:, rows] = dg
        return 0

    lax.fori_loop(0, a.shape[0] // chunk, one, 0)

    def two(i, _):
        cols = pl.ds(pl.multiple_of(i * n_out, n_out), n_out)
        ac, dc = a[:, cols], dh[:, cols]
        pg[cols, :] = jnp.dot(dgt[...], ac, preferred_element_type=F32).T
        pu[cols, :] = jnp.dot(dut[...], ac, preferred_element_type=F32).T
        pd[:, cols] = jnp.dot(hid[...], dc, preferred_element_type=F32)
        return 0

    def three(i, _):
        cols = pl.ds(pl.multiple_of(i * n_out, n_out), n_out)
        da[0][:, cols] += jnp.dot(wg[0], dgt[:, cols], preferred_element_type=F32) + jnp.dot(wu[0], dut[:, cols], preferred_element_type=F32)
        return 0

    if da:
        lax.fori_loop(0, a.shape[0] // n_out, three, 0)

    lax.fori_loop(0, a.shape[1] // n_out, two, 0)


def own_grads(number, a, dh, w, want_da, skip=0, ffb=640, chunk=1024, n_out=1024):
    rows, d = a.shape
    ff = w[0].shape[2]
    whole = pl.BlockSpec((rows, d), lambda f: (0, 0), pipeline_mode=pl.Buffered(1))
    w_in = [pl.BlockSpec((1, d, ffb), lambda f: (number, 0, f + skip))] * 2 + [pl.BlockSpec((1, ffb, d), lambda f: (number, f + skip, 0))]
    out = [pl.BlockSpec((d, ffb), lambda f: (0, f + skip))] * 2 + [pl.BlockSpec((ffb, d), lambda f: (f + skip, 0))]
    out_shape = [jax.ShapeDtypeStruct(one.shape[1:], F32) for one in w]
    out += [pl.BlockSpec((ffb, d), lambda f: (f + skip, 0))] * 2
    out_shape += [jax.ShapeDtypeStruct((ff, d), BF16)] * 2
    if want_da:
        out, out_shape = out + [pl.BlockSpec((d, rows), lambda f: (0, 0))], out_shape + [jax.ShapeDtypeStruct((d, rows), F32)]
    blocks = ff // ffb - skip
    return pl.pallas_call(
        functools.partial(own_kernel, chunk, n_out),
        grid=(blocks,),
        in_specs=[whole, whole] + w_in,
        out_specs=out,
        out_shape=out_shape,
        scratch_shapes=[pltpu.VMEM((ffb, rows), BF16)] * 3,
        compiler_params=pltpu.CompilerParams(vmem_limit_bytes=67_043_328, dimension_semantics=("arbitrary",)),
        cost_estimate=pl.CostEstimate(flops=(16 if want_da else 12) * rows * d * ffb * blocks, bytes_accessed=18 * d * ffb * blocks, transcendentals=0),
    )(a, dh, *w)


def matmul(a, w):
    return jnp.dot(a, w, preferred_element_type=F32).astype(BF16)


def scale_of(h):
    wide = h.astype(F32)
    return lax.rsqrt(jnp.mean(wide**2, -1, keepdims=True) + 1e-6)


def own_chain(x, w):
    gate0, up0, down0 = w
    a0 = (x.astype(F32) * scale_of(x)).astype(BF16)
    g, u = jnp.dot(a0, gate0, preferred_element_type=F32), jnp.dot(a0, up0, preferred_element_type=F32)
    h = x + matmul((jax.nn.silu(g) * u).astype(BF16), down0)
    scale = scale_of(h)
    wide = h.astype(F32)
    a1 = (wide * scale).astype(BF16)
    return a0, h, a1, scale


def own_back(h, scale, da, dy):
    wide, da = h.astype(F32), da.astype(BF16).astype(F32)
    back = da * scale - wide * (scale * scale * scale) * jnp.mean(da * wide, -1, keepdims=True)
    return dy + back.astype(BF16)


BLOCK, SHARED = 640, 2


def solution(mesh):
    n = mesh.shape["dp"]
    assert SHARED * BLOCK // n * 2 == BLOCK

    def step(x, dy, *arrays):
        w, m, v = (arrays[i : i + 3] for i in (0, 3, 6))
        x, dy = x[0], dy[0]

        def gather(one):
            return lax.all_gather(one, "dp", tiled=True)

        a0, h1, a1, scale = own_chain(x, tuple(one[0] for one in w))
        dy_all = gather(dy)
        a1_all = gather(a1)
        *parts1, gate1, up1, da = own_grads(1, a1, dy, w, True)
        dh1 = own_back(h1, scale, da.T, dy)
        *parts0, gate0, up0 = own_grads(0, a0, dh1, w, False, skip=SHARED)
        a0, _ = lax.optimization_barrier((a0, a1))
        a0_all, dh1_all = gather(a0), gather(dh1)
        others = lambda i: lax.rem(lax.axis_index("dp") + 1 + i, n)
        each = SHARED * BLOCK // n
        start = lax.axis_index("dp") * each
        gate, up = (lax.dynamic_slice(one, (0, 0, start), (1, one.shape[1], each))[0].T for one in w[:2])
        down = lax.dynamic_slice(w[2], (0, start, 0), (1, each, w[2].shape[2]))[0]
        new = layer_step(1, a1_all, dy_all, (n - 1, x.shape[0], others, others), (gate1, up1), w, m, v, base=parts1, after=parts0[:1])
        a0_all, *new = lax.optimization_barrier((a0_all, *new))
        mine = part_grads(a0_all, dh1_all, gate, up, down, n)
        grads = gather(mine)
        new = layer_step(0, a0_all, dh1_all, (n - 1, x.shape[0], others, others), (gate0, up0), w, m, v, base=parts0, done=new, skip=SHARED, after=(mine,))
        return tuple(update_step(0, grads, w, m, v, new, SHARED))

    return jax.shard_map(
        step,
        mesh=mesh,
        in_specs=(P(("rep", "dp"), None, None),) * 2 + (P(None, None, None),) * 9,
        out_specs=(P("rep", None, None),) * 9,
        check_vma=False,
    )
```
